128 devices in a mesh: rep: 4 (over x, y), seq: 16 (over z), tp: 2 (over core).
Axes of the slice: x: 2, y: 2, z: 16, core: 2. Of those that a mesh axis runs over, the one named last changes fastest.
The devices are a block of a 8x8x16 slice.
Arguments:
- prefill_query: bfloat16 [32768, 2048], P(('rep', 'seq'), 'tp'), parts along dimension 0, may hold values from -50 to 50
- prefill_key: bfloat16 [32768, 512], P(('rep', 'seq'), 'tp'), parts along dimension 0, may hold values from -6 to 6
- prefill_value: bfloat16 [32768, 512], P(('rep', 'seq'), 'tp'), parts along dimension 0, may hold values from -6 to 6
- doc_ids: int32 [32768], P('rep'), parts along dimension 0, may hold values from 0 to 3, never falling along the last dimension, each value on 1 to 4096 neighbouring positions
- head_window: int32 [16], P('tp'), may hold values from 1024 to 4096, as said below
- dec_query: bfloat16 [256, 2048], P('rep', 'tp'), parts along dimension 0, may hold values from -50 to 50
- dec_key: bfloat16 [256, 512], P('rep', 'tp'), parts along dimension 0, may hold values from -6 to 6
- dec_value: bfloat16 [256, 512], P('rep', 'tp'), parts along dimension 0, may hold values from -6 to 6
- cache_key: bfloat16 [262144, 512], P(('rep', 'seq'), 'tp'), parts along dimension 0, may hold values from -6 to 6
- cache_value: bfloat16 [262144, 512], P(('rep', 'seq'), 'tp'), parts along dimension 0, may hold values from -6 to 6
- page_order: int32 [2048], P(('rep', 'seq')), parts along dimension 0, may hold values from 0 to 511, each once
- lengths: int32 [256], P('rep'), parts along dimension 0, may hold values from 1 to 1024, 32768 in all
- out_proj: bfloat16 [2048, 4096], P('tp'), may hold values from -0.125 to 0.125
Outputs:
- prompt_out: bfloat16 [32768, 4096], P(('rep', 'seq', 'tp')), parts along dimension 0
- decode_out: bfloat16 [256, 4096], P(('rep', 'tp')), parts along dimension 0
The draws below stay inside these ranges and needn't reach their ends.
There are 4 independent parts, one for each index of `rep`. The reference program is written for one: setup_inputs(seed, part) draws one part's arguments, and reference() takes and returns one part's arrays. A program takes and returns all parts, laid end to end along the dimension named above; an argument that names none is the same for every part. Nothing has to cross between parts.
Inputs may be any that keep to these rules, and one draw needn't show every extreme that they name: `head_window`: some head has window 4096.
All inputs are finite; a program needn't handle non-finite values.
Results may differ from the reference program's by a relative error of at most 0.015.
Values may be sent and summed in bfloat16 or wider, within the bound.
A program may use at most 256 MiB of HBM per device.

```python
import math
import jax
import jax.numpy as jnp
import numpy as np
from jax import lax

D = 4096
HD = 128
HEADS = 16
KV_HEADS = 4
WINDOW = 4096
REQS = 64
PAGE = 128
TOKENS = 8192
PAGES = 512
MAXLEN = 1024
N_TP = 2


def prompt_keys(key):
    base = jax.random.fold_in(key, 7)
    keys = jnp.clip(jax.random.normal(base, (TOKENS, KV_HEADS * HD), jnp.float32), -6.0, 6.0)
    return keys


def draw_prefill_key(key, part):
    return prompt_keys(key).astype(jnp.bfloat16)


def draw_prefill_query(key, part):
    base = jax.random.fold_in(key, 8)
    queries = jnp.clip(jax.random.normal(base, (TOKENS, HEADS * HD), jnp.float32), -6.0, 6.0)
    return queries.astype(jnp.bfloat16)


def decode_keys(key):
    base = jax.random.fold_in(key, 9)
    keys = jnp.clip(jax.random.normal(base, (REQS, KV_HEADS * HD), jnp.float32), -6.0, 6.0)
    return keys


def draw_dec_key(key, part):
    return decode_keys(key).astype(jnp.bfloat16)


def draw_dec_query(key, part):
    base = jax.random.fold_in(key, 10)
    queries = jnp.clip(jax.random.normal(base, (REQS, HEADS * HD), jnp.float32), -6.0, 6.0)
    return queries.astype(jnp.bfloat16)


def draw_head_window(key, part):
    widths = jax.random.randint(jax.random.fold_in(key, 3), (HEADS,), WINDOW // 4, WINDOW + 1)
    picked = jax.random.randint(jax.random.fold_in(key, 4), (), 0, HEADS)
    return jnp.where(jnp.arange(HEADS) == picked, WINDOW, widths).astype(jnp.int32)


def shard_levels(key, shape, split, least, largest):
    factor_of, own = 1.0, jax.random.fold_in(key, 6)
    for dim, parts in split:
        draws = jnp.exp(jax.random.uniform(jax.random.fold_in(own, dim), (parts,), jnp.float32, least / len(split), largest / len(split)))
        factor_of = factor_of * jnp.repeat(draws, shape[dim] // parts).reshape([-1 if axis == dim else 1 for axis in range(len(shape))])
    return factor_of


def length_profile(count, total, most, skew):
    weights = [(1 << 20) // math.isqrt(grade ** skew) + 1 for grade in range(2, count + 1)]
    spare, holding = total - most - (count - 1), [1] * (count - 1)
    while spare > 0:
        free = [i for i in range(count - 1) if holding[i] < most]
        mass, budget = sum([weights[i] for i in free]), spare
        for i in free:
            extra = min(most - holding[i], max(1, budget * weights[i] // mass), spare)
            holding[i] = holding[i] + extra
            spare = spare - extra
    return np.array([most] + holding)


def uneven(stream_key, count, total, bound, lean):
    if count == 2:
        one = jax.random.randint(stream_key, (), max(1, total - bound), min(bound, total - 1) + 1)
        return jnp.stack([one, total - one])
    tallies = jnp.asarray(length_profile(count, total, bound, lean), jnp.int32)
    pairs = (count - 1) // 2
    source_of, taker = tallies[1:1 + 2 * pairs:2], tallies[2:2 + 2 * pairs:2]
    margin = jnp.minimum(source_of - 1, bound - taker)
    passed = jax.random.randint(jax.random.fold_in(stream_key, 1), (pairs,), 0, 1 << 20) % (margin + 1)
    tallies = tallies.at[1:1 + 2 * pairs:2].set(source_of - passed).at[2:2 + 2 * pairs:2].set(taker + passed)
    return tallies[jax.random.permutation(jax.random.fold_in(stream_key, 2), count)]


def normal_values(key, extent, scale, bound, pieces=(), kind=jnp.bfloat16):
    level = shard_levels(key, extent, pieces, -0.22, 0.18) if pieces else 1.0
    entries = jax.random.normal(key, extent, jnp.float32) * scale * level
    return jnp.minimum(jnp.maximum(entries, -bound), bound).astype(kind)


def setup_inputs(seed: int = 0, part: int = 0) -> dict:
    streams_of = jax.random.split(jax.random.key(seed), 14)
    part_keys = jax.random.split(jax.random.fold_in(streams_of[13], part), 14)
    return {
        "prefill_query": draw_prefill_query(jax.random.fold_in(jax.random.fold_in(streams_of[13], part), 71), part),
        "prefill_key": draw_prefill_key(jax.random.fold_in(jax.random.fold_in(streams_of[13], part), 71), part),
        "prefill_value": normal_values(part_keys[2], (TOKENS, KV_HEADS * HD), 1.0, 6.0, ((0, 16), (1, 2))),
        "doc_ids": jnp.searchsorted(jnp.cumsum(uneven(part_keys[3], 4, TOKENS, TOKENS // 2, 1)), jnp.arange(TOKENS), side="right").astype(jnp.int32),
        "head_window": draw_head_window(jax.random.fold_in(streams_of[13], 71), part),
        "dec_query": draw_dec_query(jax.random.fold_in(jax.random.fold_in(streams_of[13], part), 71), part),
        "dec_key": draw_dec_key(jax.random.fold_in(jax.random.fold_in(streams_of[13], part), 71), part),
        "dec_value": normal_values(part_keys[7], (REQS, KV_HEADS * HD), 1.0, 6.0, ((1, 2),)),
        "cache_key": normal_values(part_keys[8], (PAGES * PAGE, KV_HEADS * HD), 1.0, 6.0, ((0, 16), (1, 2))),
        "cache_value": normal_values(part_keys[9], (PAGES * PAGE, KV_HEADS * HD), 1.0, 6.0, ((0, 16), (1, 2))),
        "page_order": jax.random.permutation(part_keys[10], PAGES).astype(jnp.int32),
        "lengths": uneven(part_keys[11], REQS, REQS * MAXLEN // 2, MAXLEN, 2).astype(jnp.int32),
        "out_proj": normal_values(streams_of[12], (HEADS * HD, D), (HEADS * HD) ** -0.5, 0.125, ((0, 2),)),
    }


masked_score = -1e+30

def round_half(values):
    return lax.optimization_barrier(values.astype(jnp.bfloat16)).astype(jnp.float32)

def project(rows_matrix, out_proj):
    columns = HEADS * HD // N_TP
    total = jnp.zeros((rows_matrix.shape[0], D), jnp.float32)
    for group in range(N_TP):
        partial_sum = jnp.dot(rows_matrix[:, group * columns:(group + 1) * columns], out_proj[group * columns:(group + 1) * columns], preferred_element_type=jnp.float32)
        total = total + round_half(partial_sum)
    return total.astype(jnp.bfloat16)

def reference(prefill_query, prefill_key, prefill_value, doc_ids, head_window, dec_query, dec_key, dec_value, cache_key, cache_value, page_order, lengths, out_proj):
    group_size = HEADS // KV_HEADS
    scale_factor = 1.0 / math.sqrt(HD)
    block = math.gcd(512, TOKENS)
    key_pad = jnp.pad(prefill_key, ((WINDOW, 0), (0, 0)))
    value_pad = jnp.pad(prefill_value, ((WINDOW, 0), (0, 0)))
    doc_pad = jnp.pad(doc_ids, (WINDOW, 0), constant_values=-1)
    windows = head_window.reshape(KV_HEADS, group_size)

    def one_block(index):
        start = (index * block).astype(jnp.int32)
        queries = lax.dynamic_slice_in_dim(prefill_query, start, block, 0).reshape(block, KV_HEADS, group_size, HD).astype(jnp.float32)
        keys = lax.dynamic_slice_in_dim(key_pad, start, block + WINDOW, 0).reshape(block + WINDOW, KV_HEADS, HD).astype(jnp.float32)
        values = lax.dynamic_slice_in_dim(value_pad, start, block + WINDOW, 0).reshape(block + WINDOW, KV_HEADS, HD).astype(jnp.float32)
        query_doc = lax.dynamic_slice_in_dim(doc_ids, start, block, 0)
        key_doc = lax.dynamic_slice_in_dim(doc_pad, start, block + WINDOW, 0)
        query_pos = start + jnp.arange(block, dtype=jnp.int32)
        key_pos = start - WINDOW + jnp.arange(block + WINDOW, dtype=jnp.int32)
        gap = query_pos[:, None] - key_pos[None, :]
        allowed = (gap >= 0) & (query_doc[:, None] == key_doc[None, :])
        allowed = allowed[None, None] & (gap[None, None] < windows[:, :, None, None])
        scores = jnp.einsum('tkgd,skd->kgts', queries, keys) * scale_factor
        scores = jnp.where(allowed, scores, masked_score)
        highest = lax.optimization_barrier(jnp.max(scores, axis=-1))
        weights = jnp.where(allowed, jnp.exp(scores - highest[..., None]), 0.0)
        totals = lax.optimization_barrier(jnp.sum(weights, axis=-1))
        output = jnp.einsum('kgts,skd->kgtd', round_half(weights), values) / totals[..., None]
        return output.transpose(2, 0, 1, 3).reshape(block, HEADS * HD).astype(jnp.bfloat16)
    prompt_attn = lax.map(one_block, jnp.arange(TOKENS // block, dtype=jnp.int32)).reshape(TOKENS, HEADS * HD)
    prompt_out = project(prompt_attn, out_proj)
    inverse = jnp.zeros((PAGES,), jnp.int32).at[page_order].set(jnp.arange(PAGES, dtype=jnp.int32))
    cached_keys = cache_key.reshape(PAGES, PAGE, KV_HEADS * HD)[inverse].reshape(REQS, MAXLEN, KV_HEADS, HD).astype(jnp.float32)
    cached_values = cache_value.reshape(PAGES, PAGE, KV_HEADS * HD)[inverse].reshape(REQS, MAXLEN, KV_HEADS, HD).astype(jnp.float32)
    queries = dec_query.reshape(REQS, KV_HEADS, group_size, HD).astype(jnp.float32)
    own_keys = dec_key.reshape(REQS, KV_HEADS, HD).astype(jnp.float32)
    own_values = dec_value.reshape(REQS, KV_HEADS, HD).astype(jnp.float32)
    scores = jnp.einsum('rkgd,rskd->rkgs', queries, cached_keys) * scale_factor
    valid = (jnp.arange(MAXLEN, dtype=jnp.int32)[None, :] < lengths[:, None])[:, None, None, :]
    scores = jnp.where(valid, scores, masked_score)
    own_scores = jnp.einsum('rkgd,rkd->rkg', queries, own_keys) * scale_factor
    highest = jnp.maximum(lax.optimization_barrier(jnp.max(scores, axis=-1)), own_scores)
    weights = jnp.where(valid, jnp.exp(scores - highest[..., None]), 0.0)
    own_weights = jnp.exp(own_scores - highest)
    totals = lax.optimization_barrier(jnp.sum(weights, axis=-1)) + own_weights
    output = jnp.einsum('rkgs,rskd->rkgd', round_half(weights), cached_values) + round_half(own_weights)[..., None] * own_values[:, :, None, :]
    decode_attn = (output / totals[..., None]).reshape(REQS, HEADS * HD).astype(jnp.bfloat16)
    decode_out = project(decode_attn, out_proj)
    return (prompt_out, decode_out)
```

```python
import functools
import math

import jax
import jax.numpy as jnp
from jax import lax
from jax.experimental import pallas as pl
from jax.experimental.pallas import tpu as pltpu
from jax.sharding import PartitionSpec as P

HD = 128
PAGE = 128
MASKED = -1e30
START = -1e29
MESH = pl.DeviceIdType.MESH


def lane_iota(rows):
    return lax.broadcasted_iota(jnp.int32, (rows, 128), 1)


def row_iota(rows):
    return lax.broadcasted_iota(jnp.int32, (rows, 128), 0)


def attention_kernel(
    n,
    q_ref, k_ref, v_ref, doc_ref, hw_ref, dq_ref, dk_ref, dv_ref, ck_hbm, cv_hbm, po_ref, len_ref, w_hbm,
    out_hbm, dout_ref,
    q2_ref, lo_ref, m_ref, l_ref, acc_ref,
    fkv, bkv,
    ck_ref, cv_ref, dq2_ref, dm_ref, dl_ref, dacc_ref,
    obuf, lbuf, orecv, lrecv, dgat,
    w_ref, attn, sent, got, held,
    cache_sem, w_sem, p_send, p_recv, out_sem, f_send, f_recv, b_send, b_recv, a_send, a_recv,
    r_send, r_recv, s_send, s_recv,
):
    me = lax.axis_index("seq")
    core = lax.axis_index("tp")
    right = lax.rem(me + 1, n)
    left = lax.rem(me + n - 1, n)
    tok = q_ref.shape[0]
    heads = q_ref.shape[1] // HD
    kv = k_ref.shape[1] // HD
    group = heads // kv
    reqs = dq_ref.shape[0]
    pages = po_ref.shape[0]
    slots = pages * n // reqs
    hops, front = fkv.shape[1:3]
    legs, back = bkv.shape[1:3]
    piece = front // 2
    drows = reqs * group
    half = tok // 2
    share = drows // n
    scale = math.log2(math.e) / math.sqrt(HD)
    nt = (((1,), (1,)), ((), ()))

    caches = [
        pltpu.make_async_copy(ck_hbm, ck_ref, cache_sem.at[0]),
        pltpu.make_async_copy(cv_hbm, cv_ref, cache_sem.at[1]),
    ]
    for copy in caches:
        copy.start()
    weights_copy = pltpu.make_async_copy(w_hbm, w_ref, w_sem.at[0])
    weights_copy.start()

    barrier = pltpu.get_barrier_semaphore()

    @pl.loop(1, n)
    def _(off):
        pl.semaphore_signal(
            barrier, inc=1, device_id={"seq": lax.rem(me + off, n)}, device_id_type=MESH
        )

    pl.semaphore_signal(barrier, inc=1, device_id={"tp": 1 - core}, device_id_type=MESH)
    pl.semaphore_wait(barrier, n)

    def remote(src, dst, send, recv, to):
        return pltpu.make_async_remote_copy(
            src_ref=src, dst_ref=dst, send_sem=send, recv_sem=recv,
            device_id={"seq": to}, device_id_type=MESH,
        )

    def f_copy(d, u, own=None):
        rows = pl.ds(pl.multiple_of(u // 2 * piece, 16), piece)
        w = lax.rem(u, 2)
        src = fkv.at[w, d - 2, rows] if own is None else own.at[rows]
        return remote(src, fkv.at[w, d - 1, rows], f_send.at[d - 1, u], f_recv.at[d - 1, u], right)

    skip = n - 1 - hops

    def b_copy(h, w):
        return remote(bkv.at[w, h - 2], bkv.at[w, h - 1], b_send.at[h - 1, w], b_recv.at[h - 1, w], left)

    def b_first(w):
        src = (k_ref, v_ref)[w].at[pl.ds(front, back)]
        to = lax.rem(me + n - skip, n)
        return remote(src, bkv.at[w, 0], b_send.at[0, w], b_recv.at[0, w], to)

    for w in range(2):
        b_first(w).start()
    for u in range(4):
        f_copy(1, u, (k_ref, v_ref)[u % 2]).start()

    doc = doc_ref[...]
    row = row_iota(tok)
    qpos = row + me * tok
    first_key = jnp.zeros((tok, 128), jnp.int32)
    for value in range(1, 4):
        below = jnp.where(doc < value, 1.0, 0.0)
        count = jnp.sum(jnp.sum(below, axis=0, keepdims=True), axis=1, keepdims=True)
        begin = jnp.broadcast_to(count, (tok, 128)).astype(jnp.int32)
        first_key = jnp.where(qpos >= begin, begin, first_key)

    def halves(x):
        x = x.astype(jnp.float32) * scale
        high = x.astype(jnp.bfloat16)
        return high, (x - high.astype(jnp.float32)).astype(jnp.bfloat16)

    for h in range(heads):
        rows = pl.ds(h * tok, tok)
        q2_ref[rows, :HD], q2_ref[rows, HD:] = halves(q_ref[:, h * HD : (h + 1) * HD])
        lo_ref[rows] = jnp.maximum(first_key, qpos - hw_ref[h] + 1)
    m_ref[...] = jnp.full(m_ref.shape, START, jnp.float32)
    l_ref[...] = jnp.zeros(l_ref.shape, jnp.float32)
    acc_ref[...] = jnp.zeros(acc_ref.shape, jnp.float32)
    for h in range(heads):
        rows = pl.ds(h * reqs, reqs)
        dq2_ref[rows, :HD], dq2_ref[rows, HD:] = halves(dq_ref[:, h * HD : (h + 1) * HD])
    dm_ref[...] = jnp.full(dm_ref.shape, START, jnp.float32)
    dl_ref[...] = jnp.zeros(dl_ref.shape, jnp.float32)
    dacc_ref[...] = jnp.zeros(dacc_ref.shape, jnp.float32)

    def fold(q2, k, v, masks, m_at, l_at, acc_at):
        keys = k.shape[0]
        s = lax.dot_general(
            q2, jnp.concatenate([k, k], axis=1), nt, preferred_element_type=jnp.float32
        )
        parts = [
            jnp.where(masks[c], s[:, c * 128 : (c + 1) * 128], MASKED) for c in range(keys // 128)
        ]
        top = functools.reduce(jnp.maximum, parts)
        old = m_at[...]
        new = jnp.maximum(old, jnp.max(top, axis=1, keepdims=True))
        alpha = jnp.exp2(old - new)
        weights = [jnp.exp2(part - new) for part in parts]
        m_at[...] = new
        l_at[...] = l_at[...] * alpha + functools.reduce(jnp.add, weights)
        p = jnp.concatenate([w.astype(jnp.bfloat16) for w in weights], axis=1)
        acc_at[...] = acc_at[...] * alpha + jnp.dot(p, v, preferred_element_type=jnp.float32)

    lane = lane_iota(1)
    wide_lane = lane_iota(tok)

    def columns_of(g):
        return pl.ds(pl.multiple_of(g * HD, HD), HD)

    def prompt_fold(j, k, v, places, causal=False):
        for i in range(pair):
            rows = pl.ds(pl.multiple_of((j * pair + i) * tok, tok), tok)
            low = lo_ref[rows]
            masks = []
            for c, place in enumerate(places):
                ok = place >= low
                if causal:
                    ok = ok & (wide_lane + c * 128 <= row)
                masks.append(ok)
            fold(q2_ref[rows], k, v, masks, m_ref.at[rows], l_ref.at[rows], acc_ref.at[rows])

    pair = heads // 4
    per = group // pair

    def own_piece(j):
        places = [lane + (me * tok + c * 128) for c in range(tok // 128)]
        g = j // per
        prompt_fold(j, k_ref[:, head_cols(g)], v_ref[:, head_cols(g)], places, True)

    def placed(starts):
        total = sum(count for count, _ in starts)
        places = []
        for c in range(-(-total // 128)):
            place, at = jnp.full((1, 128), -1, jnp.int32), total
            for count, begin in reversed(starts):
                at -= count
                if at < (c + 1) * 128 and at + count > c * 128:
                    place = jnp.where(lane + c * 128 < at + count, lane + (c * 128 - at) + begin, place)
            places.append(place)
        return places

    def joined(blocks):
        empty = -sum(block.shape[0] for block in blocks) % 128
        return jnp.concatenate(blocks + [jnp.zeros((empty, HD), jnp.bfloat16)], axis=0)

    def tile(j, d, h=None):
        cols = columns_of(j // per)
        starts = [(front, (me - d) * tok)]
        blocks = [[fkv[w, d - 1, :, cols]] for w in range(2)]
        if h is not None:
            for i in range(2):
                starts.append((back, (me - (legs + 1 - h - i)) * tok + front))
                for w in range(2):
                    blocks[w].append(bkv[w, h - 1 + i, :, cols])
        prompt_fold(j, joined(blocks[0]), joined(blocks[1]), placed(starts))

    def head_cols(g):
        return slice(g * HD, (g + 1) * HD)

    dlane = lane_iota(drows)
    drequest = lax.rem(row_iota(drows), reqs)
    step_pages = pages // 8

    def decode_tile(t):
        masks = []
        for i in range(step_pages):
            slot = po_ref[t * step_pages + i]
            owner = slot // slots
            limit = len_ref[owner] - (slot - owner * slots) * PAGE
            masks.append((drequest == owner) & (dlane < limit))
        keys = pl.ds(pl.multiple_of(t * (step_pages * PAGE), PAGE), step_pages * PAGE)
        for g in range(kv):
            rows = pl.ds(g * drows, drows)
            fold(
                dq2_ref[rows], ck_ref[keys, head_cols(g)], cv_ref[keys, head_cols(g)], masks,
                dm_ref.at[rows], dl_ref.at[rows], dacc_ref.at[rows],
            )

    both = kv * share
    diagonal = lane_iota(both) == row_iota(both)

    def a_copies(to, frm):
        return [
            remote(obuf.at[to], orecv.at[frm], a_send.at[to, 0], a_recv.at[frm, 0], to),
            remote(lbuf.at[to], lrecv.at[frm], a_send.at[to, 1], a_recv.at[frm, 1], to),
        ]

    def decode_send():
        for to in range(n):
            outs, tops = [], []
            for g in range(kv):
                rows = pl.ds(g * drows + to * share, share)
                total = jnp.sum(dl_ref[rows], axis=1, keepdims=True)
                some = total > 0.0
                outs.append(jnp.where(some, dacc_ref[rows] / jnp.where(some, total, 1.0), 0.0))
                tops.append(
                    jnp.where(some, dm_ref[rows] + jnp.log2(jnp.where(some, total, 1.0)), MASKED)
                )
            obuf[to] = jnp.concatenate(outs, axis=0).astype(jnp.bfloat16)
            tops = jnp.where(diagonal, jnp.concatenate(tops, axis=0), 0.0)
            lbuf[to] = jnp.sum(tops, axis=0, keepdims=True)
        orecv[me] = obuf[me]
        lrecv[me] = lbuf[me]

    def decode_start():
        @pl.loop(1, n)
        def _(off):
            for copy in a_copies(lax.rem(me + off, n), me):
                copy.start()

    def r_copy(t):
        block = dgat.at[lax.rem(me + n - (t - 1), n)]
        return remote(block, block, r_send.at[t - 1], r_recv.at[t - 1], right)

    def s_copy(t):
        block = dgat.at[lax.rem(me + (t - 1), n)]
        return remote(block, block, s_send.at[t - 1], s_recv.at[t - 1], left)

    def r_arrived(t):
        block = dgat.at[lax.rem(me + n - t, n)]
        remote(block, block, r_send.at[t - 1], r_recv.at[t - 1], right).wait_recv()

    def s_arrived(t):
        block = dgat.at[lax.rem(me + t, n)]
        remote(block, block, s_send.at[t - 1], s_recv.at[t - 1], left).wait_recv()

    def decode_merge():
        @pl.loop(1, n)
        def _(off):
            other = lax.rem(me + off, n)
            for copy in a_copies(other, other):
                copy.wait_recv()
            for copy in a_copies(other, me):
                copy.wait_send()

        tops = []
        for i in range(n):
            spread = jnp.broadcast_to(lrecv[i, 0:1, :], (both, 128))
            tops.append(jnp.sum(jnp.where(diagonal, spread, 0.0), axis=1, keepdims=True))
        request = pl.ds(pl.multiple_of(lax.rem(me * share, reqs), 16), share)
        own_scores, own_values = [], []
        for g in range(kv):
            rows = pl.ds(pl.multiple_of(g * drows + me * share, 16), share)
            q = dq2_ref[rows, :HD].astype(jnp.float32) + dq2_ref[rows, HD:].astype(jnp.float32)
            key = dk_ref[request, head_cols(g)].astype(jnp.float32)
            own_scores.append(jnp.sum(q * key, axis=1, keepdims=True))
            own_values.append(dv_ref[request, head_cols(g)].astype(jnp.float32))
        own_score = jnp.concatenate(own_scores, axis=0)
        peak = functools.reduce(jnp.maximum, tops + [own_score])
        total = jnp.exp2(own_score - peak)
        value = total * jnp.concatenate(own_values, axis=0)
        for i in range(n):
            w = jnp.exp2(tops[i] - peak)
            total = total + w
            value = value + w * orecv[i].astype(jnp.float32)
        dgat[me] = (value / total).astype(jnp.bfloat16)

    far_right, far_left = n // 2, n - 1 - n // 2

    def gather_hop(t):
        r_arrived(t)

        @pl.when(t < far_right)
        def _():
            r_copy(t + 1).start()

        @pl.when(t <= far_left)
        def _():
            s_arrived(t)

            @pl.when(t < far_left)
            def _():
                s_copy(t + 1).start()

    def decode_gather():
        for i in range(n):
            hh, request = divmod(i * share, reqs)
            side, request = divmod(request, reqs // 2)
            for g in range(kv):
                attn[
                    side, pl.ds(half + request, share), pl.ds((g * group + hh) * HD, HD)
                ] = dgat[i, pl.ds(g * share, share)]

    def f_pass(d, u):
        w = lax.rem(u, 2)
        block = fkv.at[w, d - 1, pl.ds(pl.multiple_of(u // 2 * piece, 16), piece)]
        remote(block, block, f_send.at[d - 1, u], f_recv.at[d - 1, u], right).wait_recv()

        @pl.when(d < hops)
        def _():
            f_copy(d + 1, u).start()

    def b_pass(h, w):
        block = bkv.at[w, h - 1]
        remote(block, block, b_send.at[h - 1, w], b_recv.at[h - 1, w], left).wait_recv()

        @pl.when(h < legs)
        def _():
            b_copy(h + 1, w).start()

    for copy in caches:
        copy.wait()
    for half_tiles in range(2):

        @pl.loop(half_tiles * 4, half_tiles * 4 + 4)
        def _(t):
            decode_tile(t)

        f_pass(1, half_tiles)
    for j in range(2):
        own_piece(j)
        f_pass(1, 2 + j)
    decode_send()
    own_piece(2)
    decode_start()
    own_piece(3)

    lag = hops // 2

    @pl.loop(2, hops + 2)
    def _(d):
        @pl.loop(0, 4)
        def _(j):
            @pl.when(d <= hops)
            def _():
                f_pass(d, j)
                h = 2 * (d - lag) + j // 2

                @pl.when(h >= 1)
                def _():
                    b_pass(h, lax.rem(j, 2))

            @pl.when((d >= 4) & (d < 4 + far_right // 2) & (lax.rem(j, 2) == 0))
            def _():
                gather_hop((d - 4) * 2 + j // 2 + 1)

            @pl.when(d <= lag + 1)
            def _():
                tile(j, d - 1)

            @pl.when(d > lag + 1)
            def _():
                tile(j, d - 1, 2 * (d - lag - 1))

            @pl.when((d == 3) & (j == 2))
            def _():
                decode_merge()

            @pl.when((d == 3) & (j == 3))
            def _():
                r_copy(1).start()
                s_copy(1).start()

    decode_gather()
    for w in range(2):
        b_first(w).wait_send()
    for u in range(4):
        f_copy(1, u, (k_ref, v_ref)[u % 2]).wait_send()

    @pl.loop(2, hops + 1)
    def _(d):
        @pl.loop(0, 4)
        def _(u):
            f_copy(d, u).wait_send()

    @pl.loop(2, legs + 1)
    def _(h):
        for w in range(2):
            b_copy(h, w).wait_send()

    @pl.loop(1, far_right + 1)
    def _(t):
        r_copy(t).wait_send()

    @pl.loop(1, far_left + 1)
    def _(t):
        s_copy(t).wait_send()

    for h in range(heads):
        for side in range(2):
            rows = pl.ds(h * tok + side * half, half)
            total = jnp.sum(l_ref[rows], axis=1, keepdims=True)
            attn[side, pl.ds(0, half), pl.ds(h * HD, HD)] = (acc_ref[rows] / total).astype(
                jnp.bfloat16
            )

    weights_copy.wait()
    tiles, _, wide = sent.shape

    def columns(t):
        return pl.ds(pl.multiple_of(t * wide, wide), wide)

    def part(side, t):
        return jnp.dot(attn[side], w_ref[:, columns(t)], preferred_element_type=jnp.float32)

    def p_copy(t):
        return pltpu.make_async_remote_copy(
            src_ref=sent.at[t], dst_ref=got.at[t], send_sem=p_send.at[t], recv_sem=p_recv.at[t],
            device_id={"tp": 1 - core}, device_id_type=MESH,
        )

    def out_copy(t):
        return pltpu.make_async_copy(held.at[t], out_hbm.at[:, columns(t)], out_sem.at[t])

    @pl.loop(0, tiles)
    def _(t):
        sent[t] = part(1 - core, t).astype(jnp.bfloat16)

        @pl.when(t > 0)
        def _():
            p_copy(t - 1).start()

    @pl.loop(0, tiles)
    def _(t):
        own = part(core, t)

        @pl.when(t == 0)
        def _():
            p_copy(tiles - 1).start()

        p_copy(t).wait_recv()
        total = (own + got[t].astype(jnp.float32)).astype(jnp.bfloat16)
        held[t] = total[:half]
        dout_ref[:, columns(t)] = total[half:]

        @pl.when(t > 0)
        def _():
            out_copy(t - 1).start()

    out_copy(tiles - 1).start()

    @pl.loop(0, tiles)
    def _(t):
        p_copy(t).wait_send()
        out_copy(t).wait()


def attend(q, k, v, doc, hw, dq, dk, dv, ck, cv, po, lengths, w):
    n = lax.axis_size("seq")
    tok, width = q.shape
    heads = width // HD
    kv = k.shape[1] // HD
    hops = 4096 // tok
    reqs = dq.shape[0]
    back = 160
    front = tok - back
    legs = hops + 1
    drows = heads * reqs
    share = drows // n
    half, dhalf, out_width = tok // 2, reqs // 2, w.shape[1]
    wide = 512
    tiles = out_width // wide
    bf, f32, i32 = jnp.bfloat16, jnp.float32, jnp.int32
    vm = pl.BlockSpec(memory_space=pltpu.VMEM)
    sm = pl.BlockSpec(memory_space=pltpu.SMEM)
    hbm = pl.BlockSpec(memory_space=pl.ANY)
    dma = pltpu.SemaphoreType.DMA
    return pl.pallas_call(
        functools.partial(attention_kernel, n),
        name="ring_attention",
        out_shape=(
            jax.ShapeDtypeStruct((half, out_width), bf),
            jax.ShapeDtypeStruct((dhalf, out_width), bf),
        ),
        in_specs=[vm, vm, vm, vm, sm, vm, vm, vm, hbm, hbm, sm, sm, hbm],
        out_specs=(hbm, vm),
        scratch_shapes=[
            pltpu.VMEM((heads * tok, 2 * HD), bf),
            pltpu.VMEM((heads * tok, 128), i32),
            pltpu.VMEM((heads * tok, 128), f32),
            pltpu.VMEM((heads * tok, 128), f32),
            pltpu.VMEM((heads * tok, HD), f32),
            pltpu.VMEM((2, hops, front, kv * HD), bf),
            pltpu.VMEM((2, legs, back, kv * HD), bf),
            pltpu.VMEM(ck.shape, bf),
            pltpu.VMEM(cv.shape, bf),
            pltpu.VMEM((drows, 2 * HD), bf),
            pltpu.VMEM((drows, 128), f32),
            pltpu.VMEM((drows, 128), f32),
            pltpu.VMEM((drows, HD), f32),
            pltpu.VMEM((n, share, HD), bf),
            pltpu.VMEM((n, 1, 128), f32),
            pltpu.VMEM((n, share, HD), bf),
            pltpu.VMEM((n, 1, 128), f32),
            pltpu.VMEM((n, share, HD), bf),
            pltpu.VMEM(w.shape, bf),
            pltpu.VMEM((2, half + dhalf, width), bf),
            pltpu.VMEM((tiles, half + dhalf, wide), bf),
            pltpu.VMEM((tiles, half + dhalf, wide), bf),
            pltpu.VMEM((tiles, half, wide), bf),
            dma((2,)),
            dma((1,)),
            dma((tiles,)),
            dma((tiles,)),
            dma((tiles,)),
            dma((hops, 4)),
            dma((hops, 4)),
            dma((legs, 2)),
            dma((legs, 2)),
            dma((n, 2)),
            dma((n, 2)),
            dma((n // 2,)),
            dma((n // 2,)),
            dma((n // 2,)),
            dma((n // 2,)),
        ],
        compiler_params=pltpu.CompilerParams(
            collective_id=0, has_side_effects=True, vmem_limit_bytes=60 * 1024 * 1024
        ),
    )(q, k, v, doc.reshape(-1, 128), hw, dq, dk, dv, ck, cv, po, lengths, w)


def on_device(
    prefill_query,
    prefill_key,
    prefill_value,
    doc_ids,
    head_window,
    dec_query,
    dec_key,
    dec_value,
    cache_key,
    cache_value,
    page_order,
    lengths,
    out_proj,
):
    return attend(
        prefill_query, prefill_key, prefill_value, doc_ids, head_window,
        dec_query, dec_key, dec_value, cache_key, cache_value, page_order, lengths, out_proj,
    )


def solution(mesh):
    placed = (
        P(("rep", "seq"), "tp"),
        P(("rep", "seq"), "tp"),
        P(("rep", "seq"), "tp"),
        P("rep"),
        P("tp"),
        P("rep", "tp"),
        P("rep", "tp"),
        P("rep", "tp"),
        P(("rep", "seq"), "tp"),
        P(("rep", "seq"), "tp"),
        P(("rep", "seq")),
        P("rep"),
        P("tp", None),
    )
    return jax.shard_map(
        on_device,
        mesh=mesh,
        in_specs=placed,
        out_specs=(P(("rep", "seq", "tp"), None), P(("rep", "tp"), None)),
        check_vma=False,
    )
```

```python
import functools
import math

import jax
import jax.numpy as jnp
from jax import lax
from jax.experimental import pallas as pl
from jax.experimental.pallas import tpu as pltpu
from jax.sharding import PartitionSpec as P

HD = 128
PAGE = 128
MASKED = -1e30
START = -1e29
MESH = pl.DeviceIdType.MESH


def lane_iota(rows):
    return lax.broadcasted_iota(jnp.int32, (rows, 128), 1)


def row_iota(rows):
    return lax.broadcasted_iota(jnp.int32, (rows, 128), 0)


def attention_kernel(
    n,
    q_hbm, k_ref, v_ref, doc_ref, hw_ref, dq_ref, dk_ref, dv_ref, ck_hbm, cv_hbm, po_ref, len_ref, w_hbm,
    out_ref, dout_ref,
    q_ref, q2_ref, lo_ref, m_ref, l_ref, acc_ref,
    fkv, bkv,
    ck_ref, cv_ref, dq2_ref, dm_ref, dl_ref, dacc_ref,
    obuf, lbuf, orecv, lrecv, dgat,
    w_ref, attn, sent, got,
    q_sem, cache_sem, w_sem, p_send, p_recv, f_send, f_recv, b_send, b_recv, a_send, a_recv,
    r_send, r_recv, s_send, s_recv,
):
    me = lax.axis_index("seq")
    core = lax.axis_index("tp")
    right = lax.rem(me + 1, n)
    left = lax.rem(me + n - 1, n)
    q_copy = pltpu.make_async_copy(q_hbm, q_ref, q_sem.at[0])
    q_copy.start()
    tok = q_ref.shape[0]
    heads = q_ref.shape[1] // HD
    kv = k_ref.shape[1] // HD
    group = heads // kv
    reqs = dq_ref.shape[0]
    pages = po_ref.shape[0]
    slots = pages * n // reqs
    hops, front = fkv.shape[1:3]
    legs, back = bkv.shape[1:3]
    piece = front // 2
    drows = reqs * group
    half = tok // 2
    share = drows // n
    scale = math.log2(math.e) / math.sqrt(HD)
    nt = (((1,), (1,)), ((), ()))

    caches = [
        pltpu.make_async_copy(ck_hbm, ck_ref, cache_sem.at[0]),
        pltpu.make_async_copy(cv_hbm, cv_ref, cache_sem.at[1]),
    ]
    for copy in caches:
        copy.start()
    weights_copy = pltpu.make_async_copy(w_hbm, w_ref, w_sem.at[0])

    barrier = pltpu.get_barrier_semaphore()

    @pl.loop(1, n)
    def _(off):
        pl.semaphore_signal(
            barrier, inc=1, device_id={"seq": lax.rem(me + off, n)}, device_id_type=MESH
        )

    pl.semaphore_signal(barrier, inc=1, device_id={"tp": 1 - core}, device_id_type=MESH)
    pl.semaphore_wait(barrier, n)

    def remote(src, dst, send, recv, to):
        return pltpu.make_async_remote_copy(
            src_ref=src, dst_ref=dst, send_sem=send, recv_sem=recv,
            device_id={"seq": to}, device_id_type=MESH,
        )

    def f_copy(d, u, own=None):
        rows = pl.ds(pl.multiple_of(u // 2 * piece, 16), piece)
        w = lax.rem(u, 2)
        src = fkv.at[w, d - 2, rows] if own is None else own.at[rows]
        return remote(src, fkv.at[w, d - 1, rows], f_send.at[d - 1, u], f_recv.at[d - 1, u], right)

    skip = n - 1 - hops

    def b_rows(u):
        return pl.ds(pl.multiple_of(u // 2 * (back // 2), 8), back // 2)

    def b_copy(h, u):
        w, rows = lax.rem(u, 2), b_rows(u)
        src, dst = bkv.at[w, h - 2, rows], bkv.at[w, h - 1, rows]
        return remote(src, dst, b_send.at[h - 1, u], b_recv.at[h - 1, u], left)

    def b_first(u):
        src = (k_ref, v_ref)[u % 2].at[pl.ds(front + u // 2 * (back // 2), back // 2)]
        dst = bkv.at[u % 2, 0, pl.ds(u // 2 * (back // 2), back // 2)]
        to = lax.rem(me + n - skip, n)
        return remote(src, dst, b_send.at[0, u], b_recv.at[0, u], to)

    for u in range(4):
        b_first(u).start()
    for u in range(4):
        f_copy(1, u, (k_ref, v_ref)[u % 2]).start()

    doc = doc_ref[...]
    row = row_iota(tok)
    qpos = row + me * tok
    first_key = jnp.zeros((tok, 128), jnp.int32)
    for value in range(1, 4):
        below = jnp.where(doc < value, 1.0, 0.0)
        count = jnp.sum(jnp.sum(below, axis=0, keepdims=True), axis=1, keepdims=True)
        begin = jnp.broadcast_to(count, (tok, 128)).astype(jnp.int32)
        first_key = jnp.where(qpos >= begin, begin, first_key)

    def halves(x):
        x = x.astype(jnp.float32) * scale
        high = x.astype(jnp.bfloat16)
        return high, (x - high.astype(jnp.float32)).astype(jnp.bfloat16)

    q_copy.wait()
    for h in range(heads):
        rows = pl.ds(h * tok, tok)
        q2_ref[rows, :HD], q2_ref[rows, HD:] = halves(q_ref[:, h * HD : (h + 1) * HD])
        lo_ref[rows] = jnp.maximum(first_key, qpos - hw_ref[h] + 1)
    m_ref[...] = jnp.full(m_ref.shape, START, jnp.float32)
    l_ref[...] = jnp.zeros(l_ref.shape, jnp.float32)
    acc_ref[...] = jnp.zeros(acc_ref.shape, jnp.float32)
    for h in range(heads):
        rows = pl.ds(h * reqs, reqs)
        dq2_ref[rows, :HD], dq2_ref[rows, HD:] = halves(dq_ref[:, h * HD : (h + 1) * HD])
    dm_ref[...] = jnp.full(dm_ref.shape, START, jnp.float32)
    dl_ref[...] = jnp.zeros(dl_ref.shape, jnp.float32)
    dacc_ref[...] = jnp.zeros(dacc_ref.shape, jnp.float32)

    def fold(q2, k, v, masks, m_at, l_at, acc_at):
        keys = k.shape[0]
        s = lax.dot_general(
            q2, jnp.concatenate([k, k], axis=1), nt, preferred_element_type=jnp.float32
        )
        parts = [
            jnp.where(masks[c], s[:, c * 128 : (c + 1) * 128], MASKED) for c in range(keys // 128)
        ]
        top = functools.reduce(jnp.maximum, parts)
        old = m_at[...]
        new = jnp.maximum(old, jnp.max(top, axis=1, keepdims=True))
        alpha = jnp.exp2(old - new)
        weights = [jnp.exp2(part - new) for part in parts]
        m_at[...] = new
        l_at[...] = l_at[...] * alpha + functools.reduce(jnp.add, weights)
        p = jnp.concatenate([w.astype(jnp.bfloat16) for w in weights], axis=1)
        acc_at[...] = acc_at[...] * alpha + jnp.dot(p, v, preferred_element_type=jnp.float32)

    lane = lane_iota(1)
    wide_lane = lane_iota(tok)

    def columns_of(g):
        return pl.ds(pl.multiple_of(g * HD, HD), HD)

    def prompt_fold(j, k, v, places, causal=False):
        for i in range(pair):
            rows = pl.ds(pl.multiple_of((j * pair + i) * tok, tok), tok)
            low = lo_ref[rows]
            masks = []
            for c, place in enumerate(places):
                ok = place >= low
                if causal:
                    ok = ok & (wide_lane + c * 128 <= row)
                masks.append(ok)
            fold(q2_ref[rows], k, v, masks, m_ref.at[rows], l_ref.at[rows], acc_ref.at[rows])

    pair = heads // 4
    per = group // pair

    def own_piece(j):
        places = [lane + (me * tok + c * 128) for c in range(tok // 128)]
        g = j // per
        prompt_fold(j, k_ref[:, head_cols(g)], v_ref[:, head_cols(g)], places, True)

    def placed(starts):
        total = sum(count for count, _ in starts)
        places = []
        for c in range(-(-total // 128)):
            place, at = jnp.full((1, 128), -1, jnp.int32), total
            for count, begin in reversed(starts):
                at -= count
                if at < (c + 1) * 128 and at + count > c * 128:
                    place = jnp.where(lane + c * 128 < at + count, lane + (c * 128 - at) + begin, place)
            places.append(place)
        return places

    def joined(blocks):
        empty = -sum(block.shape[0] for block in blocks) % 128
        rest = [jnp.zeros((empty, HD), jnp.bfloat16)] if empty else []
        return jnp.concatenate(blocks + rest, axis=0)

    def tile(j, d, h=None, count=0):
        cols = columns_of(j // per)
        starts = [(front, (me - d) * tok)]
        blocks = [[fkv[w, d - 1, :, cols]] for w in range(2)]
        if count:
            for i in range(count):
                starts.append((back, (me - (legs + 1 - h - i)) * tok + front))
                for w in range(2):
                    blocks[w].append(bkv[w, h - 1 + i, :, cols])
        prompt_fold(j, joined(blocks[0]), joined(blocks[1]), placed(starts))

    def head_cols(g):
        return slice(g * HD, (g + 1) * HD)

    dlane = lane_iota(drows)
    drequest = lax.rem(row_iota(drows), reqs)
    step_pages = pages // 8

    def decode_tile(t):
        masks = []
        for i in range(step_pages):
            slot = po_ref[t * step_pages + i]
            owner = slot // slots
            limit = len_ref[owner] - (slot - owner * slots) * PAGE
            masks.append((drequest == owner) & (dlane < limit))
        keys = pl.ds(pl.multiple_of(t * (step_pages * PAGE), PAGE), step_pages * PAGE)
        for g in range(kv):
            rows = pl.ds(g * drows, drows)
            fold(
                dq2_ref[rows], ck_ref[keys, head_cols(g)], cv_ref[keys, head_cols(g)], masks,
                dm_ref.at[rows], dl_ref.at[rows], dacc_ref.at[rows],
            )

    both = kv * share
    diagonal = lane_iota(both) == row_iota(both)

    def a_copies(to, frm):
        return [
            remote(obuf.at[to], orecv.at[frm], a_send.at[to, 0], a_recv.at[frm, 0], to),
            remote(lbuf.at[to], lrecv.at[frm], a_send.at[to, 1], a_recv.at[frm, 1], to),
        ]

    def decode_send():
        for to in range(n):
            outs, tops = [], []
            for g in range(kv):
                rows = pl.ds(g * drows + to * share, share)
                total = jnp.sum(dl_ref[rows], axis=1, keepdims=True)
                some = total > 0.0
                outs.append(jnp.where(some, dacc_ref[rows] / jnp.where(some, total, 1.0), 0.0))
                tops.append(
                    jnp.where(some, dm_ref[rows] + jnp.log2(jnp.where(some, total, 1.0)), MASKED)
                )
            obuf[to] = jnp.concatenate(outs, axis=0).astype(jnp.bfloat16)
            tops = jnp.where(diagonal, jnp.concatenate(tops, axis=0), 0.0)
            lbuf[to] = jnp.sum(tops, axis=0, keepdims=True)
        orecv[me] = obuf[me]
        lrecv[me] = lbuf[me]

    def decode_start():
        @pl.loop(1, n)
        def _(off):
            for copy in a_copies(lax.rem(me + off, n), me):
                copy.start()

    def r_copy(t):
        block = dgat.at[lax.rem(me + n - (t - 1), n)]
        return remote(block, block, r_send.at[t - 1], r_recv.at[t - 1], right)

    def s_copy(t):
        block = dgat.at[lax.rem(me + (t - 1), n)]
        return remote(block, block, s_send.at[t - 1], s_recv.at[t - 1], left)

    def r_arrived(t):
        block = dgat.at[lax.rem(me + n - t, n)]
        remote(block, block, r_send.at[t - 1], r_recv.at[t - 1], right).wait_recv()

    def s_arrived(t):
        block = dgat.at[lax.rem(me + t, n)]
        remote(block, block, s_send.at[t - 1], s_recv.at[t - 1], left).wait_recv()

    def decode_merge():
        @pl.loop(1, n)
        def _(off):
            other = lax.rem(me + off, n)
            for copy in a_copies(other, other):
                copy.wait_recv()
            for copy in a_copies(other, me):
                copy.wait_send()

        tops = []
        for i in range(n):
            spread = jnp.broadcast_to(lrecv[i, 0:1, :], (both, 128))
            tops.append(jnp.sum(jnp.where(diagonal, spread, 0.0), axis=1, keepdims=True))
        request = pl.ds(pl.multiple_of(lax.rem(me * share, reqs), 16), share)
        own_scores, own_values = [], []
        for g in range(kv):
            rows = pl.ds(pl.multiple_of(g * drows + me * share, 16), share)
            q = dq2_ref[rows, :HD].astype(jnp.float32) + dq2_ref[rows, HD:].astype(jnp.float32)
            key = dk_ref[request, head_cols(g)].astype(jnp.float32)
            own_scores.append(jnp.sum(q * key, axis=1, keepdims=True))
            own_values.append(dv_ref[request, head_cols(g)].astype(jnp.float32))
        own_score = jnp.concatenate(own_scores, axis=0)
        peak = functools.reduce(jnp.maximum, tops + [own_score])
        total = jnp.exp2(own_score - peak)
        value = total * jnp.concatenate(own_values, axis=0)
        for i in range(n):
            w = jnp.exp2(tops[i] - peak)
            total = total + w
            value = value + w * orecv[i].astype(jnp.float32)
        dgat[me] = (value / total).astype(jnp.bfloat16)

    far_right, far_left = n // 2, n - 1 - n // 2

    def gather_hop(t):
        r_arrived(t)

        @pl.when(t < far_right)
        def _():
            r_copy(t + 1).start()

        @pl.when(t <= far_left)
        def _():
            s_arrived(t)

            @pl.when(t < far_left)
            def _():
                s_copy(t + 1).start()

    def decode_gather():
        for i in range(n):
            hh, request = divmod(i * share, reqs)
            side, request = divmod(request, reqs // 2)
            for g in range(kv):
                attn[
                    side, pl.ds(half + request, share), pl.ds((g * group + hh) * HD, HD)
                ] = dgat[i, pl.ds(g * share, share)]

    def f_pass(d, u):
        w = lax.rem(u, 2)
        block = fkv.at[w, d - 1, pl.ds(pl.multiple_of(u // 2 * piece, 16), piece)]
        remote(block, block, f_send.at[d - 1, u], f_recv.at[d - 1, u], right).wait_recv()

        @pl.when(d < hops)
        def _():
            f_copy(d + 1, u).start()

    def b_pass(h, u):
        block = bkv.at[lax.rem(u, 2), h - 1, b_rows(u)]
        remote(block, block, b_send.at[h - 1, u], b_recv.at[h - 1, u], left).wait_recv()

        @pl.when(h < legs)
        def _():
            b_copy(h + 1, u).start()

    own_piece(0)
    own_piece(1)
    f_pass(1, 0)
    own_piece(2)
    own_piece(3)
    f_pass(1, 1)
    for copy in caches:
        copy.wait()
    weights_copy.start()
    for u in range(2, 4):

        @pl.loop(2 * u - 4, 2 * u - 2)
        def _(t):
            decode_tile(t)

        f_pass(1, u)

    @pl.loop(4, 8)
    def _(t):
        decode_tile(t)

    decode_send()

    lag = hops // 2

    @pl.loop(2, hops + 2)
    def _(d):
        @pl.loop(0, 4)
        def _(j):
            @pl.when((d == 2) & (j == 1))
            def _():
                decode_start()

            @pl.when(d <= hops)
            def _():
                f_pass(d, j)
                h = 2 * (d - lag) + j // 2 + 1

                @pl.when((h >= 1) & (h <= legs))
                def _():
                    b_pass(h, lax.rem(j, 2) * 2)
                    b_pass(h, lax.rem(j, 2) * 2 + 1)

            @pl.when((d >= 4) & (d < 4 + far_right // 2) & (lax.rem(j, 2) == 0))
            def _():
                gather_hop((d - 4) * 2 + j // 2 + 1)

            @pl.when(d <= lag)
            def _():
                tile(j, d - 1)

            @pl.when((d == lag + 1) | (d == hops + 1))
            def _():
                tile(j, d - 1, 2 + (legs - 2) * (d // (hops + 1)), 1)

            @pl.when((d > lag + 1) & (d <= hops))
            def _():
                tile(j, d - 1, 2 * (d - lag) - 1, 2)

            @pl.when((d == 3) & (j == 2))
            def _():
                decode_merge()

            @pl.when((d == 3) & (j == 3))
            def _():
                r_copy(1).start()
                s_copy(1).start()

    decode_gather()
    for u in range(4):
        b_first(u).wait_send()
    for u in range(4):
        f_copy(1, u, (k_ref, v_ref)[u % 2]).wait_send()

    @pl.loop(2, hops + 1)
    def _(d):
        @pl.loop(0, 4)
        def _(u):
            f_copy(d, u).wait_send()

    @pl.loop(2, legs + 1)
    def _(h):
        for u in range(4):
            b_copy(h, u).wait_send()

    @pl.loop(1, far_right + 1)
    def _(t):
        r_copy(t).wait_send()

    @pl.loop(1, far_left + 1)
    def _(t):
        s_copy(t).wait_send()

    for h in range(heads):
        for side in range(2):
            rows = pl.ds(h * tok + side * half, half)
            total = jnp.sum(l_ref[rows], axis=1, keepdims=True)
            attn[side, pl.ds(0, half), pl.ds(h * HD, HD)] = (acc_ref[rows] / total).astype(
                jnp.bfloat16
            )

    weights_copy.wait()
    tiles, _, wide = sent.shape

    def columns(t):
        return pl.ds(pl.multiple_of(t * wide, wide), wide)

    def part(side, t):
        return jnp.dot(attn[side], w_ref[:, columns(t)], preferred_element_type=jnp.float32)

    def p_copy(t):
        return pltpu.make_async_remote_copy(
            src_ref=sent.at[t], dst_ref=got.at[t], send_sem=p_send.at[t], recv_sem=p_recv.at[t],
            device_id={"tp": 1 - core}, device_id_type=MESH,
        )

    @pl.loop(0, tiles)
    def _(t):
        sent[t] = part(1 - core, t).astype(jnp.bfloat16)

        @pl.when(t > 0)
        def _():
            p_copy(t - 1).start()

    @pl.loop(0, tiles)
    def _(t):
        own = part(core, t)

        @pl.when(t == 0)
        def _():
            p_copy(tiles - 1).start()

        p_copy(t).wait_recv()
        total = (own + got[t].astype(jnp.float32)).astype(jnp.bfloat16)
        out_ref[:, columns(t)] = total[:half]
        dout_ref[:, columns(t)] = total[half:]

    @pl.loop(0, tiles)
    def _(t):
        p_copy(t).wait_send()


def attend(q, k, v, doc, hw, dq, dk, dv, ck, cv, po, lengths, w):
    n = lax.axis_size("seq")
    tok, width = q.shape
    heads = width // HD
    kv = k.shape[1] // HD
    hops = 4096 // tok
    reqs = dq.shape[0]
    back = 160
    front = tok - back
    legs = hops + 1
    drows = heads * reqs
    share = drows // n
    half, dhalf, out_width = tok // 2, reqs // 2, w.shape[1]
    wide = 1024
    tiles = out_width // wide
    bf, f32, i32 = jnp.bfloat16, jnp.float32, jnp.int32
    vm = pl.BlockSpec(memory_space=pltpu.VMEM)
    sm = pl.BlockSpec(memory_space=pltpu.SMEM)
    hbm = pl.BlockSpec(memory_space=pl.ANY)
    dma = pltpu.SemaphoreType.DMA
    return pl.pallas_call(
        functools.partial(attention_kernel, n),
        name="ring_attention",
        out_shape=(
            pltpu.VMEM((half, out_width), bf),
            pltpu.VMEM((dhalf, out_width), bf),
        ),
        in_specs=[hbm, vm, vm, vm, sm, vm, vm, vm, hbm, hbm, sm, sm, hbm],
        out_specs=(vm, vm),
        scratch_shapes=[
            pltpu.VMEM((tok, width), bf),
            pltpu.VMEM((heads * tok, 2 * HD), bf),
            pltpu.VMEM((heads * tok, 128), i32),
            pltpu.VMEM((heads * tok, 128), f32),
            pltpu.VMEM((heads * tok, 128), f32),
            pltpu.VMEM((heads * tok, HD), f32),
            pltpu.VMEM((2, hops, front, kv * HD), bf),
            pltpu.VMEM((2, legs, back, kv * HD), bf),
            pltpu.VMEM(ck.shape, bf),
            pltpu.VMEM(cv.shape, bf),
            pltpu.VMEM((drows, 2 * HD), bf),
            pltpu.VMEM((drows, 128), f32),
            pltpu.VMEM((drows, 128), f32),
            pltpu.VMEM((drows, HD), f32),
            pltpu.VMEM((n, share, HD), bf),
            pltpu.VMEM((n, 1, 128), f32),
            pltpu.VMEM((n, share, HD), bf),
            pltpu.VMEM((n, 1, 128), f32),
            pltpu.VMEM((n, share, HD), bf),
            pltpu.VMEM(w.shape, bf),
            pltpu.VMEM((2, half + dhalf, width), bf),
            pltpu.VMEM((tiles, half + dhalf, wide), bf),
            pltpu.VMEM((tiles, half + dhalf, wide), bf),
            dma((1,)),
            dma((2,)),
            dma((1,)),
            dma((tiles,)),
            dma((tiles,)),
            dma((hops, 4)),
            dma((hops, 4)),
            dma((legs, 4)),
            dma((legs, 4)),
            dma((n, 2)),
            dma((n, 2)),
            dma((n // 2,)),
            dma((n // 2,)),
            dma((n // 2,)),
            dma((n // 2,)),
        ],
        compiler_params=pltpu.CompilerParams(
            collective_id=0, has_side_effects=True, vmem_limit_bytes=60 * 1024 * 1024
        ),
    )(q, k, v, doc.reshape(-1, 128), hw, dq, dk, dv, ck, cv, po, lengths, w)


def on_device(
    prefill_query,
    prefill_key,
    prefill_value,
    doc_ids,
    head_window,
    dec_query,
    dec_key,
    dec_value,
    cache_key,
    cache_value,
    page_order,
    lengths,
    out_proj,
):
    return attend(
        prefill_query, prefill_key, prefill_value, doc_ids, head_window,
        dec_query, dec_key, dec_value, cache_key, cache_value, page_order, lengths, out_proj,
    )


def solution(mesh):
    placed = (
        P(("rep", "seq"), "tp"),
        P(("rep", "seq"), "tp"),
        P(("rep", "seq"), "tp"),
        P("rep"),
        P("tp"),
        P("rep", "tp"),
        P("rep", "tp"),
        P("rep", "tp"),
        P(("rep", "seq"), "tp"),
        P(("rep", "seq"), "tp"),
        P(("rep", "seq")),
        P("rep"),
        P("tp", None),
    )
    return jax.shard_map(
        on_device,
        mesh=mesh,
        in_specs=placed,
        out_specs=(P(("rep", "seq", "tp"), None), P(("rep", "tp"), None)),
        check_vma=False,
    )
```
